32 devices in a mesh: det: 4 (over y, x), tm: 8 (over z, core).
Axes of the slice: x: 2, y: 2, z: 4, core: 2. Of those that a mesh axis runs over, the one named last changes fastest.
Arguments:
- sol_map: float32 [3, 49152], P(None, ('det', 'tm')), may hold values from -6 to 6
- resid_map: float32 [3, 49152], P(None, ('det', 'tm')), may hold values from -6 to 6
- direction: float32 [3, 49152], P(None, ('det', 'tm')), may hold values from -6 to 6
- precond: float32 [3, 49152], P(None, ('det', 'tm')), may hold values from 0.1 to 1
- pixels: int32 [128, 65536], P('det', 'tm'), may hold values from 0 to 49151
- angle_index: int32 [128, 65536], P('det', 'tm'), may hold values from 0 to 127
- angles: float32 [128], replicated, may hold values from -3.140625 to 3.140625
- flag_mask: int32 [128, 65536], P('det', 'tm'), may hold values 0 or 1
- inv_noise: float32 [128, 32769], P(('det', 'tm')), may hold values from 0.05 to 1
Outputs:
- new_sol: float32 [3, 49152], P(None, ('det', 'tm'))
- new_resid: float32 [3, 49152], P(None, ('det', 'tm'))
- new_dir: float32 [3, 49152], P(None, ('det', 'tm'))
- new_norm: float32 [], replicated
The draws below stay inside these ranges and needn't reach their ends.
All inputs are finite; a program needn't handle non-finite values. No bound on the sum of `flag_mask` on one device may be relied on, other than what follows from the above.
Results may differ from the reference program's by a relative error of at most 0.0001.
Values sent between devices are 32-bit elements; how exact they have to be, the bound alone decides.
A program may use at most 320 MiB of HBM per device.

```python
import math
import jax
import jax.numpy as jnp
from jax import lax

NSAMP = 65536
NDET = 128
NPIX = 49152
NANG = 128
NFREQ = 32769


def touch_ends(values, own_key, smallest, largest):
    shape = values.shape
    index_at = [jax.random.randint(jax.random.fold_in(own_key, axis), (), 0, shape[axis]) for axis in range(len(shape))]
    values = values.at[tuple(index_at)].set(smallest)
    longest = shape.index(max(shape))
    index_at[longest] = (index_at[longest] + 1) % shape[longest]
    return values.at[tuple(index_at)].set(largest)


def block_scale(key, dims, cuts, smallest, largest):
    def one(dim, parts):
        heights = jax.random.uniform(jax.random.fold_in(jax.random.fold_in(key, 6), dim), (parts,), jnp.float32, smallest / len(cuts), largest / len(cuts))
        return jnp.repeat(jnp.exp(heights), dims[dim] // parts).reshape((-1,) + (1,) * (len(dims) - dim - 1))

    loudness = one(*cuts[0])
    for cut in cuts[1:]:
        loudness = loudness * one(*cut)
    return loudness


def bell_draw(rng, dims, spread, limit, split=(), kind=jnp.bfloat16):
    values = jax.random.normal(rng, dims, jnp.float32) * spread
    if len(split) > 0:
        values = block_scale(rng, dims, split, -0.22, 0.18) * values
    return jnp.clip(values, min=-limit, max=limit).astype(kind)


def setup_inputs(seed: int = 0) -> dict:
    key_of = jax.random.split(jax.random.key(seed), 10)
    return {
        "sol_map": bell_draw(key_of[0], (3, NPIX), 1.0, 6.0, ((1, 32),), jnp.float32),
        "resid_map": bell_draw(key_of[1], (3, NPIX), 1.0, 6.0, ((1, 32),), jnp.float32),
        "direction": bell_draw(key_of[2], (3, NPIX), 1.0, 6.0, ((1, 32),), jnp.float32),
        "precond": jnp.clip(jnp.exp(math.log(1.0) - 2.3025851 * jax.random.uniform(key_of[3], (3, NPIX), jnp.float32) ** block_scale(key_of[3], (3, NPIX), ((1, 32),), -0.2, 0.2)), 0.1, 1.0),
        "pixels": touch_ends(jax.random.randint(key_of[4], (NDET, NSAMP), 0, NPIX), jax.random.fold_in(key_of[4], 1), 0, NPIX - 1).astype(jnp.int32),
        "angle_index": touch_ends(jax.random.randint(key_of[5], (NDET, NSAMP), 0, NANG), jax.random.fold_in(key_of[5], 1), 0, NANG - 1).astype(jnp.int32),
        "angles": jnp.clip(jax.random.uniform(key_of[6], (NANG,), jnp.float32, -3.140625, 3.140625), -3.140625, 3.140625),
        "flag_mask": touch_ends((jax.random.randint(key_of[7], (NDET, NSAMP), 0, 16) < 15).astype(jnp.int32), jax.random.fold_in(key_of[7], 1), 0, 1),
        "inv_noise": jnp.clip(jnp.exp(math.log(1.0) - 2.9957323 * jax.random.uniform(key_of[8], (NDET, NFREQ), jnp.float32) ** block_scale(key_of[8], (NDET, NFREQ), ((0, 32),), -0.2, 0.2)), 0.05, 1.0),
    }


def reference(sol_map, resid_map, direction, precond, pixels, angle_index, angles, flag_mask, inv_noise):
    cos_table = jnp.cos(2.0 * angles)
    sin_table = jnp.sin(2.0 * angles)
    row_block = 64

    def one_block(image, block_id):
        head_row = block_id * row_block
        pix_rows = lax.dynamic_slice_in_dim(pixels, head_row, row_block, 0)
        ang_rows = lax.dynamic_slice_in_dim(angle_index, head_row, row_block, 0)
        usable = lax.dynamic_slice_in_dim(flag_mask, head_row, row_block, 0).astype(jnp.float32)
        filt_rows = lax.dynamic_slice_in_dim(inv_noise, head_row, row_block, 0)
        cos_two = cos_table[ang_rows]
        sin_two = sin_table[ang_rows]
        signal = usable * (direction[0][pix_rows] + direction[1][pix_rows] * cos_two + direction[2][pix_rows] * sin_two)
        spectrum = jnp.fft.rfft(signal, axis=1)
        filtered = jnp.fft.irfft(spectrum * filt_rows, n=NSAMP, axis=1).astype(jnp.float32)
        weighted = usable * filtered
        contrib = jnp.stack([weighted, weighted * cos_two, weighted * sin_two]).reshape(3, -1)
        image = image.at[:, pix_rows.reshape(-1)].add(contrib)
        return image, None

    image, _ = lax.scan(one_block, jnp.zeros((3, NPIX), jnp.float32), jnp.arange(NDET // row_block, dtype=jnp.int32))
    norm_old = jnp.sum(resid_map * precond * resid_map)
    curvature = jnp.sum(direction * image)
    step_size = norm_old / curvature
    new_sol = sol_map + step_size * direction
    new_resid = resid_map - step_size * image
    new_norm = jnp.sum(new_resid * precond * new_resid)
    new_dir = precond * new_resid + (new_norm / norm_old) * direction
    return new_sol, new_resid, new_dir, new_norm
```

```python
import functools
import math

import jax
import jax.numpy as jnp
from jax import lax
from jax.experimental import pallas as pl
from jax.experimental.pallas import tpu as pltpu
from jax.sharding import PartitionSpec as P

LOW = 256
ROWS = 8
LANES = 128
WIDTH = 1024
CHUNKS = 2
CHUNKS_BACK = 1
TOP = 400.0
STEP = 16.0
F8 = jnp.float8_e4m3fn
BF16 = jnp.bfloat16


def product(form, left, right, precision=lax.Precision.HIGH):
    return jnp.einsum(form, left, right, precision=precision)


def lookup(table_row, index):
    rows, width = index.shape
    table = jnp.broadcast_to(table_row, (rows, LANES))
    parts = []
    for start in range(0, width, LANES):
        parts.append(jnp.take_along_axis(table, index[:, start : start + LANES], axis=1, mode="promise_in_bounds"))
    return jnp.concatenate(parts, axis=1)


def scale_of(values):
    return TOP / jnp.maximum(jnp.max(jnp.abs(values)), 1e-30)


def three_pieces(values):
    first = values.astype(F8).astype(jnp.float32)
    rest = values - first
    second = rest.astype(F8).astype(jnp.float32)
    return first, second, (rest - second) * STEP


def wide_row(row, rows, dtype):
    row = jnp.broadcast_to(row, (rows, row.shape[1]))
    return row.astype(jnp.float32).astype(dtype)


def select_tree(parts, bits):
    level = 0
    while len(parts) > 1:
        pairs = [jnp.where(bits[level], parts[i + 1], parts[i]) for i in range(0, len(parts) - 1, 2)]
        if len(parts) % 2:
            pairs.append(parts[-1])
        parts = pairs
        level += 1
    return parts[0]


def hot_pair(row, size):
    width = row.shape[1]
    ids = wide_row(lax.broadcasted_iota(jnp.int32, (16, width), 0), 16, BF16)
    same = wide_row(row & 15, 16, BF16) == ids
    group = wide_row(row >> 4, 16, BF16)
    zero = jnp.zeros((16, width), BF16)
    out = []
    for level in (1.0, 1.0 / STEP):
        base = jnp.where(same, jnp.full((16, width), level, BF16), zero)
        parts = [jnp.where(group == BF16(k), base, zero) for k in range(size // 16)]
        out.append(jnp.concatenate(parts, axis=0).astype(F8))
    return out


def hot_pair_8(row, size):
    width = row.shape[1]
    ids = lax.broadcasted_iota(jnp.int32, (32, width), 0).astype(jnp.int8)
    same = jnp.broadcast_to(row & 31, (32, width)).astype(jnp.int8) == ids
    group = jnp.broadcast_to(row >> 5, (32, width)).astype(jnp.int8)
    zero = jnp.zeros((32, width), F8)
    masks = [group == jnp.int8(k) for k in range(size // 32)]
    out = []
    for level in (1.0, 1.0 / STEP):
        base = jnp.where(same, jnp.full((32, width), level, F8), zero)
        out.append(jnp.concatenate([jnp.where(mask, base, zero) for mask in masks], axis=0))
    return out


def read_kernel(trig_ref, table_ref, pix_ref, ang_ref, flag_ref, out_ref, split_ref, scale_ref, *, high):
    @pl.when(pl.program_id(0) * pl.num_programs(1) + pl.program_id(1) == 0)
    def _():
        table = table_ref[...]
        scale = scale_of(table)
        scale_ref[0] = 1.0 / scale
        for k, piece in enumerate(three_pieces(table * scale)):
            split_ref[:, k * LOW : (k + 1) * LOW] = piece.astype(F8)

    cos_two = lookup(trig_ref[0:1, :], ang_ref[...])
    sin_two = lookup(trig_ref[1:2, :], ang_ref[...])
    usable = flag_ref[...].astype(jnp.float32) * scale_ref[0]
    pix = pix_ref[...]
    pix_low = pix & (LOW - 1)
    pix_high = pix >> (LOW.bit_length() - 1)
    width = pix.shape[1]
    ids = lax.broadcasted_iota(jnp.int32, (8, width), 0)
    count = high // 8
    for row in range(ROWS):
        one, small = hot_pair(pix_low[row : row + 1], LOW)
        hot = jnp.concatenate([one, one, small], axis=0)
        got = jnp.dot(split_ref[...], hot, preferred_element_type=jnp.float32)
        upper = jnp.broadcast_to(pix_high[row : row + 1], (8, width))
        bits = [(upper & (8 << level)) != 0 for level in range((count - 1).bit_length())]
        picks = []
        for stokes in range(3):
            start = stokes * high
            picks.append(select_tree([got[start + 8 * k : start + 8 * k + 8] for k in range(count)], bits))
        mixed = picks[0] + picks[1] * cos_two[row : row + 1] + picks[2] * sin_two[row : row + 1]
        picked = jnp.sum(jnp.where(ids == (upper & 7), mixed, 0.0), axis=0, keepdims=True)
        out_ref[row : row + 1, :] = picked * usable[row : row + 1]


def bin_kernel(trig_ref, scale_ref, pix_ref, ang_ref, flag_ref, val_ref, out_ref, *, high):
    @pl.when(pl.program_id(0) * pl.num_programs(1) + pl.program_id(1) == 0)
    def _():
        out_ref[...] = jnp.zeros_like(out_ref)

    cos_two = lookup(trig_ref[0:1, :], ang_ref[...])
    sin_two = lookup(trig_ref[1:2, :], ang_ref[...])
    weighted = flag_ref[...].astype(jnp.float32) * (val_ref[...] * scale_ref[0])
    pieces = [three_pieces(stokes) for stokes in (weighted, weighted * cos_two, weighted * sin_two)]
    pix = pix_ref[...]
    pix_low = pix & (LOW - 1)
    pix_high = pix >> (LOW.bit_length() - 1)
    width = pix.shape[1]
    ids = lax.broadcasted_iota(jnp.int32, (32, width), 0).astype(jnp.int8)
    zero = jnp.zeros((32, width), F8)
    total = None
    for row in range(ROWS):
        one, small = hot_pair_8(pix_low[row : row + 1], LOW)
        upper = pix_high[row : row + 1]
        same = jnp.broadcast_to(upper & 31, (32, width)).astype(jnp.int8) == ids
        group = jnp.broadcast_to(upper >> 5, (32, width)).astype(jnp.int8)
        masks = [group == jnp.int8(k) for k in range(high // 32)]
        columns = []
        for part in range(3):
            stack = []
            for stokes in range(3):
                value = pieces[stokes][part][row : row + 1]
                base = jnp.where(same, jnp.broadcast_to(value, (32, width)).astype(F8), zero)
                stack += [jnp.where(mask, base, zero) for mask in masks]
            columns.append(jnp.concatenate(stack, axis=0))
        left = jnp.concatenate(columns, axis=1)
        right = jnp.concatenate([one, one, small], axis=1)
        got = lax.dot_general(left, right, (((1,), (1,)), ((), ())), preferred_element_type=jnp.float32)
        total = got if total is None else total + got
    out_ref[...] += total


def cost(samples, cells):
    return pl.CostEstimate(flops=6 * 3 * samples * cells, bytes_accessed=16 * samples, transcendentals=0)


def read_map(trig, table, pixels, angle_index, flag_mask, chunk, chunks):
    n_det, n_samp = pixels.shape
    high = table.shape[0] // 3
    span = n_samp // chunks
    width = min(max(256, min(WIDTH, WIDTH * 192 // high)), span)
    steps = span // width
    block = pl.BlockSpec((ROWS, width), lambda i, j: (i, j + chunk * steps))
    fixed = lambda shape: pl.BlockSpec(shape, lambda i, j: (0, 0))
    return pl.pallas_call(
        functools.partial(read_kernel, high=high),
        out_shape=jax.ShapeDtypeStruct((n_det, span), jnp.float32),
        grid=(n_det // ROWS, steps),
        in_specs=[fixed(trig.shape), fixed(table.shape), block, block, block],
        out_specs=pl.BlockSpec((ROWS, width), lambda i, j: (i, j)),
        scratch_shapes=[pltpu.VMEM((3 * high, 3 * LOW), F8), pltpu.SMEM((1,), jnp.float32)],
        compiler_params=pltpu.CompilerParams(dimension_semantics=("arbitrary", "arbitrary")),
        cost_estimate=cost(n_det * span, high * LOW),
        name="read_map",
    )(trig, table, pixels, angle_index, flag_mask)


def bin_map(trig, pixels, angle_index, flag_mask, values, high, chunk, chunks):
    n_det, n_samp = pixels.shape
    span = n_samp // chunks
    width = min(max(256, min(WIDTH, WIDTH * 192 // high)), span)
    steps = span // width
    scale = scale_of(values).reshape(1)
    block = pl.BlockSpec((ROWS, width), lambda i, j: (i, j + chunk * steps))
    fixed = lambda shape: pl.BlockSpec(shape, lambda i, j: (0, 0))
    binned = pl.pallas_call(
        functools.partial(bin_kernel, high=high),
        out_shape=jax.ShapeDtypeStruct((3 * high, LOW), jnp.float32),
        grid=(n_det // ROWS, steps),
        in_specs=[
            fixed(trig.shape),
            pl.BlockSpec(memory_space=pltpu.SMEM),
            block,
            block,
            block,
            pl.BlockSpec((ROWS, width), lambda i, j: (i, j)),
        ],
        out_specs=fixed((3 * high, LOW)),
        compiler_params=pltpu.CompilerParams(dimension_semantics=("arbitrary", "arbitrary")),
        cost_estimate=cost(n_det * span, high * LOW),
        name="bin_map",
    )(trig, scale, pixels, angle_index, flag_mask, values)
    return binned / scale[0]


def mirrored(filt, side_len):
    n_series, half_len = filt.shape
    rows = (half_len - 1) // side_len
    lower = filt[:, : half_len - 1].reshape(n_series, rows, side_len)
    shifted = filt[:, 1:].reshape(n_series, rows, side_len)
    swap_col = jnp.flip(jnp.eye(side_len, dtype=jnp.float32), 0)
    swap_row = jnp.flip(jnp.eye(rows, dtype=jnp.float32), 0)
    exact = lax.Precision.HIGHEST
    upper = product("wv,dvk->dwk", swap_row, product("dvk,kl->dvl", shifted, swap_col, exact), exact)
    return jnp.concatenate([lower, upper], axis=1)


def noise_weight(series, filt):
    n_series, total_len = series.shape
    side_len = math.isqrt(total_len)
    indices = jnp.arange(side_len, dtype=jnp.int32)
    products = indices[:, None] * indices[None, :]
    angle_tab = 2.0 * math.pi / side_len * (products % side_len).astype(jnp.float32)
    f_real = jnp.cos(angle_tab)
    f_imag = -jnp.sin(angle_tab)
    twist = products.astype(jnp.float32) * (2.0 * math.pi / total_len)
    w_real = jnp.cos(twist)
    w_imag = -jnp.sin(twist)
    matrix_form = series.reshape(n_series, side_len, side_len)
    y_real = product("kt,dtu->dku", f_real, matrix_form)
    y_imag = product("kt,dtu->dku", f_imag, matrix_form)
    y_real, y_imag = (y_real * w_real - y_imag * w_imag, y_real * w_imag + y_imag * w_real)
    z_real = product("dku,uv->dvk", y_real, f_real) - product("dku,uv->dvk", y_imag, f_imag)
    z_imag = product("dku,uv->dvk", y_real, f_imag) + product("dku,uv->dvk", y_imag, f_real)
    weight = mirrored(filt, side_len)
    z_real = z_real * weight
    z_imag = z_imag * weight
    v_real = product("dvk,vu->dku", z_real, f_real) + product("dvk,vu->dku", z_imag, f_imag)
    v_imag = product("dvk,vu->dku", z_imag, f_real) - product("dvk,vu->dku", z_real, f_imag)
    v_real, v_imag = (v_real * w_real + v_imag * w_imag, v_imag * w_real - v_real * w_imag)
    result = product("tk,dku->dtu", f_real, v_real) + product("tk,dku->dtu", f_imag, v_imag)
    return (result / total_len).reshape(n_series, total_len)


def body(sol_map, resid_map, direction, precond, pixels, angle_index, angles, flag_mask, inv_noise):
    everyone = ("det", "tm")
    share_len = direction.shape[1]
    n_dev = lax.axis_size(everyone)
    copies = jnp.broadcast_to(direction.reshape(1, -1, LANES), (n_dev, direction.size // LANES, LANES))
    gathered = lax.all_to_all(copies, everyone, split_axis=0, concat_axis=0, tiled=True)
    high = n_dev * share_len // LOW
    table = jnp.swapaxes(gathered.reshape(n_dev, 3, share_len), 0, 1).reshape(3 * high, LOW)
    trig = jnp.stack([jnp.cos(2.0 * angles), jnp.sin(2.0 * angles)])
    n_tm = lax.axis_size("tm")
    n_det, n_samp = pixels.shape
    chunks = max(1, min(CHUNKS, n_samp // WIDTH))
    span = n_samp // chunks
    pieces = []
    for chunk in range(chunks):
        signal = read_map(trig, table, pixels, angle_index, flag_mask, chunk, chunks)
        signal = signal.reshape(n_tm, n_det // n_tm, span)
        pieces.append(lax.all_to_all(signal, "tm", split_axis=0, concat_axis=0, tiled=True))
    stacked = jnp.stack(pieces, axis=1)
    by_detector = jnp.moveaxis(stacked, 2, 0).reshape(n_det // n_tm, n_tm * n_samp)
    filtered = noise_weight(by_detector, inv_noise)
    chunks = min(CHUNKS_BACK, chunks)
    span = n_samp // chunks
    parts = jnp.moveaxis(filtered.reshape(n_det // n_tm, n_tm, chunks, span), 0, 2)
    partial_map = 0.0
    for chunk in range(chunks):
        returned = lax.all_to_all(parts[:, chunk], "tm", split_axis=0, concat_axis=0, tiled=True)
        returned = returned.reshape(n_det, span)
        partial_map += bin_map(trig, pixels, angle_index, flag_mask, returned, high, chunk, chunks)
    by_owner = jnp.swapaxes(partial_map.reshape(3, n_dev, share_len), 0, 1)
    image = jnp.sum(lax.all_to_all(by_owner, everyone, split_axis=0, concat_axis=0, tiled=True), axis=0)
    scaled_resid = precond * resid_map
    own_sums = jnp.stack(
        [
            jnp.sum(scaled_resid * resid_map),
            jnp.sum(direction * image),
            jnp.sum(image * scaled_resid),
            jnp.sum(image * precond * image),
        ]
    )
    sum_copies = jnp.broadcast_to(own_sums[None], (n_dev, own_sums.shape[0]))
    all_sums = lax.all_to_all(sum_copies, everyone, split_axis=0, concat_axis=0, tiled=True)
    norm_old, curvature, cross_term, image_norm = jnp.sum(all_sums, axis=0)
    step_size = norm_old / curvature
    new_resid = resid_map - step_size * image
    new_norm = norm_old - 2.0 * step_size * cross_term + step_size * step_size * image_norm
    new_sol = sol_map + step_size * direction
    new_dir = precond * new_resid + new_norm / norm_old * direction
    return (new_sol, new_resid, new_dir, new_norm)


def solution(mesh):
    in_specs = (
        P(None, ("det", "tm")),
        P(None, ("det", "tm")),
        P(None, ("det", "tm")),
        P(None, ("det", "tm")),
        P("det", "tm"),
        P("det", "tm"),
        P(),
        P("det", "tm"),
        P(("det", "tm"), None),
    )
    out_specs = (P(None, ("det", "tm")), P(None, ("det", "tm")), P(None, ("det", "tm")), P())
    return jax.shard_map(body, mesh=mesh, in_specs=in_specs, out_specs=out_specs, check_vma=False)
```
